32 devices in a mesh: row: 8 (over z, x), col: 4 (over y, core).
Axes of the slice: x: 2, y: 2, z: 4, core: 2. Of those that a mesh axis runs over, the one named last changes fastest.
Arguments:
- src_points: float32 [64, 8192], P(None, ('row', 'col')), as said below
- tgt_points: float32 [64, 16384], P(None, ('col', 'row')), as said below
- log_a: float32 [8192], P('row'), may hold values from -5 to 5
- log_b: float32 [16384], P('col'), may hold values from -5 to 5
- g_current: float32 [16384], P(('col', 'row')), may hold values from -4 to 4
- hist_g: float32 [4, 16384], P(None, ('col', 'row')), may hold values from -4 to 4
- hist_maps: float32 [4, 16384], P(None, ('col', 'row')), may hold values from -4 to 4
Outputs:
- f_out: float32 [8192], P('row')
- g_out: float32 [16384], P(('col', 'row'))
The draws below stay inside these ranges and needn't reach their ends.
Inputs may be any that keep to these rules, and one draw needn't show every extreme that they name: `src_points`: coordinates of the source points. `tgt_points`: coordinates of the target points.
All inputs are finite; a program needn't handle non-finite values.
Results may differ from the reference program's by a relative error of at most 0.0003.
Values sent between devices are 32-bit elements; how exact they have to be, the bound alone decides.
A program may use at most 64 MiB of HBM per device.

```python
import math
import jax
import jax.numpy as jnp
from jax import lax

D = 64
HIST = 5
ITERS = 2
N = 8192
M = 16384


def target_cloud(key):
    base = jax.random.normal(jax.random.fold_in(key, 7), (D, M), jnp.float32)
    return base * 0.15


def draw_tgt_points(key, part):
    return target_cloud(key)


def draw_src_points(key, part):
    base = jax.random.normal(jax.random.fold_in(key, 3), (D, N), jnp.float32)
    return base * 0.15


def level_of(rng, dims, pieces, smallest, top_value):
    factor_of = 1.0
    for axis_at, shards_of in pieces:
        draws = jax.random.uniform(jax.random.fold_in(jax.random.fold_in(rng, 6), axis_at), (shards_of,), jnp.float32, smallest / len(pieces), top_value / len(pieces))
        factor_of = factor_of * jnp.repeat(jnp.exp(draws), dims[axis_at] // shards_of).reshape((-1,) + (1,) * (len(dims) - 1 - axis_at))
    return factor_of


def bell_draw(own_key, shape, width, limit, cuts=(), kind=jnp.bfloat16):
    values = width * jax.random.normal(own_key, shape, jnp.float32)
    if cuts:
        values = values * level_of(own_key, shape, cuts, -0.22, 0.18)
    return jnp.clip(values, -limit, limit).astype(kind)


def setup_inputs(seed: int = 0) -> dict:
    keys = jax.random.split(jax.random.key(seed), 8)
    src_points = draw_src_points(jax.random.fold_in(keys[7], 71), 0)
    tgt_points = draw_tgt_points(jax.random.fold_in(keys[7], 71), 0)
    log_a = bell_draw(keys[2], (N,), 1.0, 5.0, ((0, 8),), jnp.float32)
    log_b = bell_draw(keys[3], (M,), 1.0, 5.0, ((0, 4),), jnp.float32)
    g_current = bell_draw(keys[4], (M,), 0.3, 4.0, ((0, 32),), jnp.float32)
    hist_g = bell_draw(keys[5], (HIST - 1, M), 0.3, 4.0, ((1, 32),), jnp.float32)
    hist_maps = bell_draw(keys[6], (HIST - 1, M), 0.3, 4.0, ((1, 32),), jnp.float32)
    return dict(src_points=src_points, tgt_points=tgt_points, log_a=log_a, log_b=log_b, g_current=g_current, hist_g=hist_g, hist_maps=hist_maps)


EPS = 0.1


def cost_of(source, source_sq, target, target_sq):
    cross = lax.dot_general(source, target, (((0,), (0,)), ((), ())), precision=lax.Precision.HIGHEST, preferred_element_type=jnp.float32)
    return source_sq[:, None] + target_sq[None, :] - 2.0 * cross


def solve_small(matrix, rhs):
    extent = matrix.shape[0]
    rows_list = [matrix[k] for k in range(extent)]
    values = [rhs[k] for k in range(extent)]
    for pivot_index in range(extent):
        for lower_row in range(pivot_index + 1, extent):
            factor = rows_list[lower_row][pivot_index] / rows_list[pivot_index][pivot_index]
            rows_list[lower_row] = rows_list[lower_row] - factor * rows_list[pivot_index]
            values[lower_row] = values[lower_row] - factor * values[pivot_index]
    answer = [None] * extent
    for pivot_index in reversed(range(extent)):
        running = values[pivot_index]
        for upper_col in range(pivot_index + 1, extent):
            running = running - rows_list[pivot_index][upper_col] * answer[upper_col]
        answer[pivot_index] = running / rows_list[pivot_index][pivot_index]
    return jnp.stack(answer)


def mix_weights(gram):
    extent = gram.shape[0]
    shift = 0.001 * jnp.trace(gram) / extent + 1e-6
    system = gram + shift * jnp.eye(extent, dtype=jnp.float32)
    weights = solve_small(system, jnp.ones((extent,), jnp.float32))
    return weights / jnp.sum(weights)


def reference(src_points, tgt_points, log_a, log_b, g_current, hist_g, hist_maps):
    source_sq = jnp.sum(src_points * src_points, axis=0)
    target_sq = jnp.sum(tgt_points * tgt_points, axis=0)
    total_rows = src_points.shape[1]
    total_cols = tgt_points.shape[1]
    row_block = math.gcd(total_rows, 1024)
    col_block = math.gcd(total_cols, 1024)

    def row_potential(g_whole):
        column_term = g_whole / EPS + log_b

        def one_block(index):
            start = (index * row_block).astype(jnp.int32)
            source = lax.dynamic_slice_in_dim(src_points, start, row_block, 1)
            sq_piece = lax.dynamic_slice_in_dim(source_sq, start, row_block, 0)
            scores = column_term[None, :] - cost_of(source, sq_piece, tgt_points, target_sq) / EPS
            top = jnp.max(scores, axis=1)
            return -EPS * (top + jnp.log(jnp.sum(jnp.exp(scores - top[:, None]), axis=1)))

        return lax.map(one_block, jnp.arange(total_rows // row_block, dtype=jnp.int32)).reshape(-1)

    def column_potential(f_whole):
        row_term = f_whole / EPS + log_a

        def one_block(index):
            start = (index * col_block).astype(jnp.int32)
            target = lax.dynamic_slice_in_dim(tgt_points, start, col_block, 1)
            sq_piece = lax.dynamic_slice_in_dim(target_sq, start, col_block, 0)
            scores = row_term[:, None] - cost_of(src_points, source_sq, target, sq_piece) / EPS
            top = jnp.max(scores, axis=0)
            return -EPS * (top + jnp.log(jnp.sum(jnp.exp(scores - top[None, :]), axis=0)))

        return lax.map(one_block, jnp.arange(total_cols // col_block, dtype=jnp.int32)).reshape(-1)

    potentials = [hist_g[k] for k in range(hist_g.shape[0])]
    images = [hist_maps[k] for k in range(hist_maps.shape[0])]
    g_whole = g_current
    f_whole = None
    for turn_index in range(ITERS):
        f_whole = row_potential(g_whole)
        mapped = column_potential(f_whole)
        potentials = (potentials + [g_whole])[-HIST:]
        images = (images + [mapped])[-HIST:]
        image_stack = jnp.stack(images)
        resid = image_stack - jnp.stack(potentials)
        gram = jnp.dot(resid, resid.T, precision=lax.Precision.HIGHEST, preferred_element_type=jnp.float32)
        mix = mix_weights(gram)
        g_whole = jnp.dot(mix, image_stack, precision=lax.Precision.HIGHEST, preferred_element_type=jnp.float32)
    return f_whole, g_whole
```

```python
import functools
import math

import jax
import jax.numpy as jnp
from jax import lax
from jax.experimental import pallas as pl
from jax.experimental.pallas import tpu as pltpu
from jax.sharding import PartitionSpec as P

MESH = pl.DeviceIdType.MESH
HIST = 5
ITERS = 2
EPS = 0.1
LOG2E = math.log2(math.e)
INV = LOG2E / EPS
BACK = EPS * math.log(2.0)
LANES = 128
F32 = jnp.float32
BF16 = jnp.bfloat16


def rounded(value):
    return value.astype(BF16).astype(F32)


def split3(value):
    first = rounded(value)
    second = rounded(value - first)
    return first, second, rounded(value - first - second)


def select_rows(shape, rows):
    at = lax.broadcasted_iota(jnp.int32, shape, 0)
    out = jnp.zeros(shape, F32)
    for index, row in rows:
        out = jnp.where(at == index, row, out)
    return out


def solve_small(rows_list, values):
    extent = len(values)
    rows_list = [list(row) for row in rows_list]
    values = list(values)
    for pivot in range(extent):
        for lower in range(pivot + 1, extent):
            factor = rows_list[lower][pivot] / rows_list[pivot][pivot]
            for at in range(pivot, extent):
                rows_list[lower][at] = rows_list[lower][at] - factor * rows_list[pivot][at]
            values[lower] = values[lower] - factor * values[pivot]
    answer = [None] * extent
    for pivot in reversed(range(extent)):
        running = values[pivot]
        for upper in range(pivot + 1, extent):
            running = running - rows_list[pivot][upper] * answer[upper]
        answer[pivot] = running / rows_list[pivot][pivot]
    return answer


def kernel(
    R, C,
    src_ref, tgt_ref, la_ref, lb_ref, g_ref, hg_ref, hm_ref,
    f_ref, gout_ref,
    src_all, tgt_all, g_all, hm_all, xt, xlow, y_all, ysq, mrow, srow,
    rp_send, rp_all, cp_send, cp_all, mp_send, mp_all, gc_send, gc_all,
    s_src, r_src, s_tgt, r_tgt, s_g, r_g, s_hm, r_hm,
    s_rp, r_rp, s_cp, r_cp, s_mp, r_mp, s_gc, r_gc,
):
    row = lax.axis_index("row")
    col = lax.axis_index("col")
    depth, nsrc = src_ref.shape
    ntgt = tgt_ref.shape[1]
    nrow = C * nsrc
    kdim = 4 * depth
    itile = min(256, nrow)
    pending = []

    def to_row(k):
        return lax.rem(row + k, R)

    def to_col(k):
        return lax.rem(col + k, C)

    def send(src, dst, ssem, rsem, device):
        copy = pltpu.make_async_remote_copy(
            src_ref=src, dst_ref=dst, send_sem=ssem, recv_sem=rsem,
            device_id=device, device_id_type=MESH,
        )
        copy.start()
        pending.append(copy)

    def arrived(dst, ssem, rsem):
        pltpu.make_async_remote_copy(
            src_ref=dst, dst_ref=dst, send_sem=ssem, recv_sem=rsem,
            device_id=(row, col), device_id_type=MESH,
        ).wait_recv()

    for k in range(1, C):
        p = to_col(k)
        send(src_ref, src_all.at[col], s_src.at[p], r_src.at[col], (row, p))
    for k in range(1, R):
        p = to_row(k)
        send(g_ref, g_all.at[row], s_g.at[p], r_g.at[row], (p, col))
        send(tgt_ref, tgt_all.at[row], s_tgt.at[p], r_tgt.at[row], (p, col))
    for k in range(1, R):
        p = to_row(k)
        send(hm_ref, hm_all.at[row], s_hm.at[p], r_hm.at[row], (p, col))

    src_all[col] = src_ref[...]
    tgt_all[row] = tgt_ref[...]
    g_all[row] = g_ref[...]
    hm_all[row] = hm_ref[...]

    def build_x(c):
        x = src_all[c]
        scaled = x * (2.0 * INV)
        high = rounded(scaled)
        low = rounded(scaled - high)
        ones = select_rows((depth, nsrc), [(k, 1.0) for k in range(3)])
        whole = jnp.concatenate([high, high, low, ones], axis=0).T.astype(BF16)
        at = pl.ds(pl.multiple_of(c * nsrc, nsrc), nsrc)
        xt[0, at, :] = whole
        xt[1, at, :] = whole
        xlow[c] = low
        return jnp.sum(x * x, axis=0, keepdims=True)

    def bias_y(p, g):
        bias = INV * g + LOG2E * lb_ref[pl.ds(p, 1), :] - INV * ysq[p]
        b1, b2, b3 = split3(bias)
        rows = [(0, b1), (1, b2), (2, b3)] + [(k, 1.0) for k in range(3, 6)]
        y_all[p, 3 * depth : 3 * depth + 16, :] = select_rows((16, ntgt), rows).astype(BF16)

    def build_y(p):
        y = tgt_all[p]
        high = y.astype(BF16)
        low = (y - high.astype(F32)).astype(BF16)
        y_all[p, 0:depth, :] = high
        y_all[p, depth : 2 * depth, :] = low
        y_all[p, 2 * depth : 3 * depth, :] = high
        y_all[p, 3 * depth + 16 :, :] = jnp.zeros((depth - 16, ntgt), BF16)
        ysq[p] = jnp.sum(y * y, axis=0, keepdims=True)
        bias_y(p, g_all[p])

    def row_chunk(p):
        for it in range(nrow // itile):
            at = slice(it * itile, (it + 1) * itile)
            s = jnp.dot(xt[0, at, :], y_all[p], preferred_element_type=F32)
            pieces = [s[:, k : k + LANES] for k in range(0, ntgt, LANES)]
            old = mrow[at, :]
            top = functools.reduce(jnp.maximum, pieces, old)
            total = srow[at, :] * jnp.exp2(old - top)
            for piece in pieces:
                total = total + jnp.exp2(piece - top)
            mrow[at, :] = top
            srow[at, :] = total

    def row_finish(turn):
        for at in range(0, nrow, LANES):
            mt = mrow[at : at + LANES, :].T
            st = srow[at : at + LANES, :].T
            top = jnp.max(mt, axis=0, keepdims=True)
            total = jnp.sum(st * jnp.exp2(mt - top), axis=0, keepdims=True)
            rp_send[turn, 0:1, at : at + LANES] = top
            rp_send[turn, 1:2, at : at + LANES] = total
        for k in range(1, C):
            p = to_col(k)
            send(rp_send.at[turn], rp_all.at[turn, col], s_rp.at[turn, p], r_rp.at[turn, col], (row, p))
        rp_all[turn, col] = rp_send[turn]
        for k in range(1, C):
            p = to_col(k)
            arrived(rp_all.at[turn, p], s_rp.at[turn, p], r_rp.at[turn, p])
        tops = [rp_all[turn, c, 0:1, :] for c in range(C)]
        top = functools.reduce(jnp.maximum, tops)
        total = jnp.zeros_like(top)
        for c in range(C):
            total = total + rp_all[turn, c, 1:2, :] * jnp.exp2(tops[c] - top)
        return top + jnp.log2(total)

    def set_row_term(lse):
        a1, a2, a3 = split3(LOG2E * la_ref[...] - lse)
        for c in range(C):
            at = slice(c * nsrc, (c + 1) * nsrc)
            rows = [(3, a1[:, at]), (4, a2[:, at]), (5, a3[:, at])]
            slab = jnp.concatenate([xlow[c], select_rows((depth, nsrc), rows)], axis=0)
            xt[1, at, 2 * depth :] = slab.T.astype(BF16)

    def col_chunk(turn, p):
        top = jnp.full((8, ntgt), -jnp.inf, F32)
        total = jnp.zeros((8, ntgt), F32)
        for it in range(nrow // itile):
            at = slice(it * itile, (it + 1) * itile)
            s = jnp.dot(xt[1, at, :], y_all[p], preferred_element_type=F32)
            s = s.reshape(itile // 8, 8, ntgt)
            new = jnp.maximum(top, jnp.max(s, axis=0))
            total = total * jnp.exp2(top - new) + jnp.sum(jnp.exp2(s - new[None]), axis=0)
            top = new
        best = jnp.max(top, axis=0, keepdims=True)
        cp_send[turn, p, 0:1, :] = best
        cp_send[turn, p, 1:2, :] = jnp.sum(total * jnp.exp2(top - best), axis=0, keepdims=True)

    def zero_bias(p, carry):
        at = lax.broadcasted_iota(jnp.int32, (16, ntgt), 0)
        one = jnp.where((at >= 3) & (at < 6), 1.0, 0.0)
        y_all[p, 3 * depth : 3 * depth + 16, :] = one.astype(BF16)
        return carry

    def reset_rows():
        mrow[...] = jnp.full(mrow.shape, -jnp.inf, F32)
        srow[...] = jnp.zeros(srow.shape, F32)

    reset_rows()
    for k in range(1, C):
        p = to_col(k)
        arrived(src_all.at[p], s_src.at[p], r_src.at[p])
    xsq = jnp.concatenate([build_x(c) for c in range(C)], axis=1)

    potentials = [hg_ref[k : k + 1, :] for k in range(hg_ref.shape[0])]
    images = [hm_ref[k : k + 1, :] for k in range(hm_ref.shape[0])]
    g_share = g_ref[...]
    own = tgt_ref[...]
    own_sq = jnp.sum(own * own, axis=0, keepdims=True)
    pairs = [(i, j) for i in range(HIST) for j in range(i, HIST)]
    grows = -(-len(pairs) // 8) * 8
    for turn in range(ITERS):
        if turn == 0:
            build_y(row)
            row_chunk(row)

            def first(k, carry):
                p = lax.rem(row + k, R)
                arrived(g_all.at[p], s_g.at[p], r_g.at[p])
                arrived(tgt_all.at[p], s_tgt.at[p], r_tgt.at[p])
                build_y(p)
                row_chunk(p)
                return carry

            lax.fori_loop(1, R, first, 0)
        else:
            reset_rows()

            def again(p, carry):
                row_chunk(p)
                return carry

            lax.fori_loop(0, R, again, 0)
        lse = row_finish(turn)
        if turn == ITERS - 1:
            f_ref[...] = xsq - BACK * lse
        set_row_term(lse)
        lax.fori_loop(0, R, zero_bias, 0)

        def cols(k, carry):
            p = lax.rem(row + k, R)
            col_chunk(turn, p)
            pltpu.make_async_remote_copy(
                src_ref=cp_send.at[turn, p], dst_ref=cp_all.at[turn, row],
                send_sem=s_cp.at[turn, p], recv_sem=r_cp.at[turn, row],
                device_id=(p, col), device_id_type=MESH,
            ).start()
            return carry

        lax.fori_loop(1, R, cols, 0)
        col_chunk(turn, row)
        cp_all[turn, row] = cp_send[turn, row]
        for k in range(1, R):
            p = to_row(k)
            arrived(cp_all.at[turn, p], s_cp.at[turn, p], r_cp.at[turn, p])
        tops = [cp_all[turn, p, 0:1, :] for p in range(R)]
        best = functools.reduce(jnp.maximum, tops)
        total = jnp.zeros_like(best)
        for p in range(R):
            total = total + cp_all[turn, p, 1:2, :] * jnp.exp2(tops[p] - best)
        mapped = own_sq - BACK * (best + jnp.log2(total))
        potentials = (potentials + [g_share])[-HIST:]
        images = (images + [mapped])[-HIST:]
        resid = [a - b for a, b in zip(images, potentials)]
        for at, (i, j) in enumerate(pairs):
            product = resid[i] * resid[j]
            mp_send[turn, at : at + 1, :] = sum(product[:, k : k + LANES] for k in range(0, ntgt, LANES))
        for at in range(len(pairs), grows):
            mp_send[turn, at : at + 1, :] = jnp.zeros((1, LANES), F32)
        for at in range(ntgt // LANES):
            mp_send[turn, grows + at : grows + at + 1, :] = mapped[:, at * LANES : (at + 1) * LANES]
        for k in range(1, R):
            p = to_row(k)
            send(mp_send.at[turn], mp_all.at[turn, row], s_mp.at[turn, p], r_mp.at[turn, row], (p, col))
        mp_all[turn, row] = mp_send[turn]
        for k in range(1, R):
            p = to_row(k)
            arrived(mp_all.at[turn, p], s_mp.at[turn, p], r_mp.at[turn, p])
        gram = mp_all[turn, 0, 0:grows, :]
        for p in range(1, R):
            gram = gram + mp_all[turn, p, 0:grows, :]
        gc_send[turn] = gram
        for k in range(1, C):
            p = to_col(k)
            send(gc_send.at[turn], gc_all.at[turn, col], s_gc.at[turn, p], r_gc.at[turn, col], (row, p))
        gc_all[turn, col] = gram
        for k in range(1, C):
            p = to_col(k)
            arrived(gc_all.at[turn, p], s_gc.at[turn, p], r_gc.at[turn, p])
        gram = gc_all[turn, 0]
        for c in range(1, C):
            gram = gram + gc_all[turn, c]
        gram = jnp.broadcast_to(jnp.sum(gram, axis=1, keepdims=True), (grows, LANES))
        system = [[None] * HIST for _ in range(HIST)]
        for at, (i, j) in enumerate(pairs):
            system[i][j] = system[j][i] = gram[at : at + 1, :]
        trace = functools.reduce(jnp.add, [system[i][i] for i in range(HIST)])
        shift = 0.001 * trace / HIST + 1e-06
        for i in range(HIST):
            system[i][i] = system[i][i] + shift
        weights = solve_small(system, [jnp.ones((1, LANES), F32)] * HIST)
        norm = functools.reduce(jnp.add, weights)
        mix = [jnp.concatenate([w / norm] * (ntgt // LANES), axis=1) for w in weights]

        def mixed(parts):
            return functools.reduce(jnp.add, [w * part for w, part in zip(mix, parts)])

        g_share = mixed(images)
        if turn < ITERS - 1:
            if turn == 0:
                for k in range(1, R):
                    p = to_row(k)
                    arrived(hm_all.at[p], s_hm.at[p], r_hm.at[p])
            for p in range(R):
                known = [hm_all[p, k : k + 1, :] for k in range(hm_ref.shape[0])]
                for past in range(turn + 1):
                    rows = [mp_all[past, p, grows + at : grows + at + 1, :] for at in range(ntgt // LANES)]
                    known.append(jnp.concatenate(rows, axis=1))
                bias_y(p, mixed(known[-HIST:]))
    gout_ref[...] = g_share
    for copy in pending:
        copy.wait_send()
    for turn in range(ITERS):
        for k in range(1, R):
            p = to_row(k)
            pltpu.make_async_remote_copy(
                src_ref=cp_send.at[turn, p], dst_ref=cp_all.at[turn, row],
                send_sem=s_cp.at[turn, p], recv_sem=r_cp.at[turn, row],
                device_id=(p, col), device_id_type=MESH,
            ).wait_send()


def shards(R, C, src, tgt, log_a, log_b, g_current, hist_g, hist_maps):
    depth, nsrc = src.shape
    ntgt = tgt.shape[1]
    nrow = C * nsrc
    nhist = hist_g.shape[0]
    pair_rows = -(-(HIST * (HIST + 1) // 2) // 8) * 8
    mp_rows = -(-(pair_rows + ntgt // LANES) // 8) * 8
    dma = pltpu.SemaphoreType.DMA
    vmem = pl.BlockSpec(memory_space=pltpu.VMEM)
    f_out, g_out = pl.pallas_call(
        functools.partial(kernel, R, C),
        out_shape=(
            jax.ShapeDtypeStruct((1, nrow), F32),
            jax.ShapeDtypeStruct((1, ntgt), F32),
        ),
        in_specs=[vmem] * 7,
        out_specs=(vmem, vmem),
        scratch_shapes=[
            pltpu.VMEM((C, depth, nsrc), F32),
            pltpu.VMEM((R, depth, ntgt), F32),
            pltpu.VMEM((R, 1, ntgt), F32),
            pltpu.VMEM((R, nhist, ntgt), F32),
            pltpu.VMEM((2, nrow, 4 * depth), BF16),
            pltpu.VMEM((C, depth, nsrc), F32),
            pltpu.VMEM((R, 4 * depth, ntgt), BF16),
            pltpu.VMEM((R, 1, ntgt), F32),
            pltpu.VMEM((nrow, LANES), F32),
            pltpu.VMEM((nrow, LANES), F32),
            pltpu.VMEM((ITERS, 2, nrow), F32),
            pltpu.VMEM((ITERS, C, 2, nrow), F32),
            pltpu.VMEM((ITERS, R, 2, ntgt), F32),
            pltpu.VMEM((ITERS, R, 2, ntgt), F32),
            pltpu.VMEM((ITERS, mp_rows, LANES), F32),
            pltpu.VMEM((ITERS, R, mp_rows, LANES), F32),
            pltpu.VMEM((ITERS, pair_rows, LANES), F32),
            pltpu.VMEM((ITERS, C, pair_rows, LANES), F32),
            dma((C,)), dma((C,)), dma((R,)), dma((R,)),
            dma((R,)), dma((R,)), dma((R,)), dma((R,)),
            dma((ITERS, C)), dma((ITERS, C)), dma((ITERS, R)), dma((ITERS, R)),
            dma((ITERS, R)), dma((ITERS, R)), dma((ITERS, C)), dma((ITERS, C)),
        ],
        compiler_params=pltpu.CompilerParams(
            has_side_effects=True, vmem_limit_bytes=48 * 1024 * 1024
        ),
    )(
        src, tgt, log_a.reshape(1, nrow), log_b.reshape(R, ntgt),
        g_current.reshape(1, ntgt), hist_g, hist_maps,
    )
    return f_out.reshape(nrow), g_out.reshape(ntgt)


def solution(mesh):
    in_specs = (
        P(None, ("row", "col")),
        P(None, ("col", "row")),
        P("row"),
        P("col"),
        P(("col", "row")),
        P(None, ("col", "row")),
        P(None, ("col", "row")),
    )
    out_specs = (P("row"), P(("col", "row")))
    body = functools.partial(shards, mesh.shape["row"], mesh.shape["col"])
    return jax.shard_map(body, mesh=mesh, in_specs=in_specs, out_specs=out_specs, check_vma=False)
```

```python
import functools
import math

import jax
import jax.numpy as jnp
from jax import lax
from jax.experimental import pallas as pl
from jax.experimental.pallas import tpu as pltpu
from jax.sharding import PartitionSpec as P

MESH = pl.DeviceIdType.MESH
HIST = 5
ITERS = 2
EPS = 0.1
LOG2E = math.log2(math.e)
INV = LOG2E / EPS
BACK = EPS * math.log(2.0)
LANES = 128
F32 = jnp.float32
BF16 = jnp.bfloat16


def rounded(value):
    return value.astype(BF16).astype(F32)


def split3(value):
    first = rounded(value)
    second = rounded(value - first)
    return first, second, rounded(value - first - second)


def select_rows(shape, rows):
    at = lax.broadcasted_iota(jnp.int32, shape, 0)
    out = jnp.zeros(shape, F32)
    for index, row in rows:
        out = jnp.where(at == index, row, out)
    return out


def solve_small(rows_list, values):
    extent = len(values)
    rows_list = [list(row) for row in rows_list]
    values = list(values)
    for pivot in range(extent):
        for lower in range(pivot + 1, extent):
            factor = rows_list[lower][pivot] / rows_list[pivot][pivot]
            for at in range(pivot, extent):
                rows_list[lower][at] = rows_list[lower][at] - factor * rows_list[pivot][at]
            values[lower] = values[lower] - factor * values[pivot]
    answer = [None] * extent
    for pivot in reversed(range(extent)):
        running = values[pivot]
        for upper in range(pivot + 1, extent):
            running = running - rows_list[pivot][upper] * answer[upper]
        answer[pivot] = running / rows_list[pivot][pivot]
    return answer


def inner_extent(R):
    best = 1
    while best * best * 4 <= R and R % (best * 2) == 0:
        best *= 2
    return best


def kernel(
    R, C,
    src_ref, tgt_ref, la_ref, lb_ref, g_ref, hg_ref, hm_ref,
    f_ref, gout_ref,
    src_all, tgt_all, g_all, hm_all, xt, xlow, y_all, ysq, mrow, srow,
    rp_send, rp_all, cp_send, cp_all, mp_send, mp_all, gc_send, gc_all,
    s_src, r_src, s_tgt, r_tgt, s_g, r_g, s_hm, r_hm,
    s_rp, r_rp, s_cp, r_cp, s_mp, r_mp, s_gc, r_gc,
):
    row = lax.axis_index("row")
    col = lax.axis_index("col")
    depth, nsrc = src_ref.shape
    ntgt = tgt_ref.shape[1]
    nrow = C * nsrc
    kdim = 4 * depth
    itile = min(256, nrow)
    pending = []

    def to_row(k):
        return lax.rem(row + k, R)

    def to_col(k):
        return lax.rem(col + k, C)

    X = inner_extent(R)
    Z = R // X
    outer, inner = row // X, lax.rem(row, X)

    def place(k, m):
        return lax.rem(outer + k, Z) * X + lax.rem(inner + m, X)

    def send(src, dst, ssem, rsem, device):
        copy = pltpu.make_async_remote_copy(
            src_ref=src, dst_ref=dst, send_sem=ssem, recv_sem=rsem,
            device_id=device, device_id_type=MESH,
        )
        copy.start()
        pending.append(copy)

    def arrived(dst, ssem, rsem):
        pltpu.make_async_remote_copy(
            src_ref=dst, dst_ref=dst, send_sem=ssem, recv_sem=rsem,
            device_id=(row, col), device_id_type=MESH,
        ).wait_recv()

    for k in range(1, C):
        p = to_col(k)
        send(src_ref, src_all.at[col], s_src.at[p], r_src.at[col], (row, p))
    for k in range(1, R):
        p = to_row(k)
        send(g_ref, g_all.at[row], s_g.at[p], r_g.at[row], (p, col))
    for k in range(1, Z):
        p = place(k, 0)
        send(tgt_ref, tgt_all.at[row], s_tgt.at[p], r_tgt.at[row], (p, col))
    for k in range(1, X):
        p = place(0, k)
        send(tgt_ref, tgt_all.at[row], s_tgt.at[p], r_tgt.at[row], (p, col))
    for k in range(1, R):
        p = to_row(k)
        send(hm_ref, hm_all.at[row], s_hm.at[p], r_hm.at[row], (p, col))

    src_all[col] = src_ref[...]
    tgt_all[row] = tgt_ref[...]
    g_all[row] = g_ref[...]
    hm_all[row] = hm_ref[...]

    def build_x(c):
        x = src_all[c]
        scaled = x * (2.0 * INV)
        high = rounded(scaled)
        low = rounded(scaled - high)
        ones = select_rows((depth, nsrc), [(k, 1.0) for k in range(3)])
        whole = jnp.concatenate([high, high, low, ones], axis=0).T.astype(BF16)
        at = pl.ds(pl.multiple_of(c * nsrc, nsrc), nsrc)
        xt[0, at, :] = whole
        xt[1, at, :] = whole
        xlow[c] = low
        return jnp.sum(x * x, axis=0, keepdims=True)

    def bias_y(p, g):
        bias = INV * g + LOG2E * lb_ref[pl.ds(p, 1), :] - INV * ysq[p]
        b1, b2, b3 = split3(bias)
        rows = [(0, b1), (1, b2), (2, b3)] + [(k, 1.0) for k in range(3, 6)]
        y_all[p, 3 * depth : 3 * depth + 16, :] = select_rows((16, ntgt), rows).astype(BF16)

    def build_y(p):
        y = tgt_all[p]
        high = y.astype(BF16)
        low = (y - high.astype(F32)).astype(BF16)
        y_all[p, 0:depth, :] = high
        y_all[p, depth : 2 * depth, :] = low
        y_all[p, 2 * depth : 3 * depth, :] = high
        y_all[p, 3 * depth + 16 :, :] = jnp.zeros((depth - 16, ntgt), BF16)
        ysq[p] = jnp.sum(y * y, axis=0, keepdims=True)
        bias_y(p, g_all[p])

    def row_chunk(p):
        for it in range(nrow // itile):
            at = slice(it * itile, (it + 1) * itile)
            s = jnp.dot(xt[0, at, :], y_all[p], preferred_element_type=F32)
            pieces = [s[:, k : k + LANES] for k in range(0, ntgt, LANES)]
            old = mrow[at, :]
            top = functools.reduce(jnp.maximum, pieces, old)
            total = srow[at, :] * jnp.exp2(old - top)
            for piece in pieces:
                total = total + jnp.exp2(piece - top)
            mrow[at, :] = top
            srow[at, :] = total

    def row_finish(turn):
        for at in range(0, nrow, LANES):
            mt = mrow[at : at + LANES, :].T
            st = srow[at : at + LANES, :].T
            top = jnp.max(mt, axis=0, keepdims=True)
            total = jnp.sum(st * jnp.exp2(mt - top), axis=0, keepdims=True)
            rp_send[turn, 0:1, at : at + LANES] = top
            rp_send[turn, 1:2, at : at + LANES] = total
        for k in range(1, C):
            p = to_col(k)
            send(rp_send.at[turn], rp_all.at[turn, col], s_rp.at[turn, p], r_rp.at[turn, col], (row, p))
        rp_all[turn, col] = rp_send[turn]
        for k in range(1, C):
            p = to_col(k)
            arrived(rp_all.at[turn, p], s_rp.at[turn, p], r_rp.at[turn, p])
        tops = [rp_all[turn, c, 0:1, :] for c in range(C)]
        top = functools.reduce(jnp.maximum, tops)
        total = jnp.zeros_like(top)
        for c in range(C):
            total = total + rp_all[turn, c, 1:2, :] * jnp.exp2(tops[c] - top)
        return top + jnp.log2(total)

    def set_row_term(lse):
        a1, a2, a3 = split3(LOG2E * la_ref[...] - lse)
        for c in range(C):
            at = slice(c * nsrc, (c + 1) * nsrc)
            rows = [(3, a1[:, at]), (4, a2[:, at]), (5, a3[:, at])]
            slab = jnp.concatenate([xlow[c], select_rows((depth, nsrc), rows)], axis=0)
            xt[1, at, 2 * depth :] = slab.T.astype(BF16)

    def col_chunk(turn, p):
        top = jnp.full((8, ntgt), -jnp.inf, F32)
        total = jnp.zeros((8, ntgt), F32)
        for it in range(nrow // itile):
            at = slice(it * itile, (it + 1) * itile)
            s = jnp.dot(xt[1, at, :], y_all[p], preferred_element_type=F32)
            s = s.reshape(itile // 8, 8, ntgt)
            new = jnp.maximum(top, jnp.max(s, axis=0))
            total = total * jnp.exp2(top - new) + jnp.sum(jnp.exp2(s - new[None]), axis=0)
            top = new
        best = jnp.max(top, axis=0, keepdims=True)
        cp_send[turn, p, 0:1, :] = best
        cp_send[turn, p, 1:2, :] = jnp.sum(total * jnp.exp2(top - best), axis=0, keepdims=True)

    def zero_bias(p, carry):
        at = lax.broadcasted_iota(jnp.int32, (16, ntgt), 0)
        one = jnp.where((at >= 3) & (at < 6), 1.0, 0.0)
        y_all[p, 3 * depth : 3 * depth + 16, :] = one.astype(BF16)
        return carry

    def reset_rows():
        mrow[...] = jnp.full(mrow.shape, -jnp.inf, F32)
        srow[...] = jnp.zeros(srow.shape, F32)

    reset_rows()
    for k in range(1, C):
        p = to_col(k)
        arrived(src_all.at[p], s_src.at[p], r_src.at[p])
    xsq = jnp.concatenate([build_x(c) for c in range(C)], axis=1)

    potentials = [hg_ref[k : k + 1, :] for k in range(hg_ref.shape[0])]
    images = [hm_ref[k : k + 1, :] for k in range(hm_ref.shape[0])]
    g_share = g_ref[...]
    own = tgt_ref[...]
    own_sq = jnp.sum(own * own, axis=0, keepdims=True)
    pairs = [(i, j) for i in range(HIST) for j in range(i, HIST)]
    grows = -(-len(pairs) // 8) * 8
    for turn in range(ITERS):
        if turn == 0:
            build_y(row)
            row_chunk(row)

            def take(p):
                arrived(g_all.at[p], s_g.at[p], r_g.at[p])
                build_y(p)
                row_chunk(p)

            def passed_on(p, q):
                return pltpu.make_async_remote_copy(
                    src_ref=tgt_all.at[p], dst_ref=tgt_all.at[p],
                    send_sem=s_tgt.at[q], recv_sem=r_tgt.at[p],
                    device_id=(row - inner + lax.rem(q, X), col),
                    device_id_type=MESH,
                )

            def first(k, carry):
                p = place(k, 0)
                arrived(tgt_all.at[p], s_tgt.at[p], r_tgt.at[p])
                for m in range(1, X):
                    passed_on(p, place(k, m)).start()
                take(p)
                return carry

            lax.fori_loop(1, Z, first, 0)

            def rest(n, carry):
                p = place(n // (X - 1), 1 + lax.rem(n, X - 1))
                arrived(tgt_all.at[p], s_tgt.at[p], r_tgt.at[p])
                take(p)
                return carry

            if X > 1:
                lax.fori_loop(0, Z * (X - 1), rest, 0)
            for k in range(1, Z):
                for m in range(1, X):
                    passed_on(place(k, 0), place(k, m)).wait_send()
        else:
            reset_rows()

            def again(p, carry):
                row_chunk(p)
                return carry

            lax.fori_loop(0, R, again, 0)
        lse = row_finish(turn)
        if turn == ITERS - 1:
            f_ref[...] = xsq - BACK * lse
        set_row_term(lse)
        lax.fori_loop(0, R, zero_bias, 0)

        def cols(k, carry):
            p = lax.rem(row + k, R)
            col_chunk(turn, p)
            pltpu.make_async_remote_copy(
                src_ref=cp_send.at[turn, p], dst_ref=cp_all.at[turn, row],
                send_sem=s_cp.at[turn, p], recv_sem=r_cp.at[turn, row],
                device_id=(p, col), device_id_type=MESH,
            ).start()
            return carry

        lax.fori_loop(1, R, cols, 0)
        col_chunk(turn, row)
        cp_all[turn, row] = cp_send[turn, row]
        for k in range(1, R):
            p = to_row(k)
            arrived(cp_all.at[turn, p], s_cp.at[turn, p], r_cp.at[turn, p])
        tops = [cp_all[turn, p, 0:1, :] for p in range(R)]
        best = functools.reduce(jnp.maximum, tops)
        total = jnp.zeros_like(best)
        for p in range(R):
            total = total + cp_all[turn, p, 1:2, :] * jnp.exp2(tops[p] - best)
        mapped = own_sq - BACK * (best + jnp.log2(total))
        potentials = (potentials + [g_share])[-HIST:]
        images = (images + [mapped])[-HIST:]
        resid = [a - b for a, b in zip(images, potentials)]
        for at, (i, j) in enumerate(pairs):
            product = resid[i] * resid[j]
            mp_send[turn, at : at + 1, :] = sum(product[:, k : k + LANES] for k in range(0, ntgt, LANES))
        for at in range(len(pairs), grows):
            mp_send[turn, at : at + 1, :] = jnp.zeros((1, LANES), F32)
        for at in range(ntgt // LANES):
            mp_send[turn, grows + at : grows + at + 1, :] = mapped[:, at * LANES : (at + 1) * LANES]
        for k in range(1, R):
            p = to_row(k)
            send(mp_send.at[turn], mp_all.at[turn, row], s_mp.at[turn, p], r_mp.at[turn, row], (p, col))
        mp_all[turn, row] = mp_send[turn]
        for k in range(1, R):
            p = to_row(k)
            arrived(mp_all.at[turn, p], s_mp.at[turn, p], r_mp.at[turn, p])
        gram = mp_all[turn, 0, 0:grows, :]
        for p in range(1, R):
            gram = gram + mp_all[turn, p, 0:grows, :]
        gc_send[turn] = gram
        for k in range(1, C):
            p = to_col(k)
            send(gc_send.at[turn], gc_all.at[turn, col], s_gc.at[turn, p], r_gc.at[turn, col], (row, p))
        gc_all[turn, col] = gram
        for k in range(1, C):
            p = to_col(k)
            arrived(gc_all.at[turn, p], s_gc.at[turn, p], r_gc.at[turn, p])
        gram = gc_all[turn, 0]
        for c in range(1, C):
            gram = gram + gc_all[turn, c]
        gram = jnp.broadcast_to(jnp.sum(gram, axis=1, keepdims=True), (grows, LANES))
        system = [[None] * HIST for _ in range(HIST)]
        for at, (i, j) in enumerate(pairs):
            system[i][j] = system[j][i] = gram[at : at + 1, :]
        trace = functools.reduce(jnp.add, [system[i][i] for i in range(HIST)])
        shift = 0.001 * trace / HIST + 1e-06
        for i in range(HIST):
            system[i][i] = system[i][i] + shift
        weights = solve_small(system, [jnp.ones((1, LANES), F32)] * HIST)
        norm = functools.reduce(jnp.add, weights)
        mix = [jnp.concatenate([w / norm] * (ntgt // LANES), axis=1) for w in weights]

        def mixed(parts):
            return functools.reduce(jnp.add, [w * part for w, part in zip(mix, parts)])

        g_share = mixed(images)
        if turn < ITERS - 1:
            if turn == 0:
                for k in range(1, R):
                    p = to_row(k)
                    arrived(hm_all.at[p], s_hm.at[p], r_hm.at[p])
            for p in range(R):
                known = [hm_all[p, k : k + 1, :] for k in range(hm_ref.shape[0])]
                for past in range(turn + 1):
                    rows = [mp_all[past, p, grows + at : grows + at + 1, :] for at in range(ntgt // LANES)]
                    known.append(jnp.concatenate(rows, axis=1))
                bias_y(p, mixed(known[-HIST:]))
    gout_ref[...] = g_share
    for copy in pending:
        copy.wait_send()
    for turn in range(ITERS):
        for k in range(1, R):
            p = to_row(k)
            pltpu.make_async_remote_copy(
                src_ref=cp_send.at[turn, p], dst_ref=cp_all.at[turn, row],
                send_sem=s_cp.at[turn, p], recv_sem=r_cp.at[turn, row],
                device_id=(p, col), device_id_type=MESH,
            ).wait_send()


def shards(R, C, src, tgt, log_a, log_b, g_current, hist_g, hist_maps):
    depth, nsrc = src.shape
    ntgt = tgt.shape[1]
    nrow = C * nsrc
    nhist = hist_g.shape[0]
    pair_rows = -(-(HIST * (HIST + 1) // 2) // 8) * 8
    mp_rows = -(-(pair_rows + ntgt // LANES) // 8) * 8
    dma = pltpu.SemaphoreType.DMA
    vmem = pl.BlockSpec(memory_space=pltpu.VMEM)
    f_out, g_out = pl.pallas_call(
        functools.partial(kernel, R, C),
        out_shape=(
            jax.ShapeDtypeStruct((1, nrow), F32),
            jax.ShapeDtypeStruct((1, ntgt), F32),
        ),
        in_specs=[vmem] * 7,
        out_specs=(vmem, vmem),
        scratch_shapes=[
            pltpu.VMEM((C, depth, nsrc), F32),
            pltpu.VMEM((R, depth, ntgt), F32),
            pltpu.VMEM((R, 1, ntgt), F32),
            pltpu.VMEM((R, nhist, ntgt), F32),
            pltpu.VMEM((2, nrow, 4 * depth), BF16),
            pltpu.VMEM((C, depth, nsrc), F32),
            pltpu.VMEM((R, 4 * depth, ntgt), BF16),
            pltpu.VMEM((R, 1, ntgt), F32),
            pltpu.VMEM((nrow, LANES), F32),
            pltpu.VMEM((nrow, LANES), F32),
            pltpu.VMEM((ITERS, 2, nrow), F32),
            pltpu.VMEM((ITERS, C, 2, nrow), F32),
            pltpu.VMEM((ITERS, R, 2, ntgt), F32),
            pltpu.VMEM((ITERS, R, 2, ntgt), F32),
            pltpu.VMEM((ITERS, mp_rows, LANES), F32),
            pltpu.VMEM((ITERS, R, mp_rows, LANES), F32),
            pltpu.VMEM((ITERS, pair_rows, LANES), F32),
            pltpu.VMEM((ITERS, C, pair_rows, LANES), F32),
            dma((C,)), dma((C,)), dma((R,)), dma((R,)),
            dma((R,)), dma((R,)), dma((R,)), dma((R,)),
            dma((ITERS, C)), dma((ITERS, C)), dma((ITERS, R)), dma((ITERS, R)),
            dma((ITERS, R)), dma((ITERS, R)), dma((ITERS, C)), dma((ITERS, C)),
        ],
        compiler_params=pltpu.CompilerParams(
            has_side_effects=True, vmem_limit_bytes=48 * 1024 * 1024
        ),
    )(
        src, tgt, log_a.reshape(1, nrow), log_b.reshape(R, ntgt),
        g_current.reshape(1, ntgt), hist_g, hist_maps,
    )
    return f_out.reshape(nrow), g_out.reshape(ntgt)


def solution(mesh):
    in_specs = (
        P(None, ("row", "col")),
        P(None, ("col", "row")),
        P("row"),
        P("col"),
        P(("col", "row")),
        P(None, ("col", "row")),
        P(None, ("col", "row")),
    )
    out_specs = (P("row"), P(("col", "row")))
    body = functools.partial(shards, mesh.shape["row"], mesh.shape["col"])
    return jax.shard_map(body, mesh=mesh, in_specs=in_specs, out_specs=out_specs, check_vma=False)
```

```python
import functools
import math

import jax
import jax.numpy as jnp
from jax import lax
from jax.experimental import pallas as pl
from jax.experimental.pallas import tpu as pltpu
from jax.sharding import PartitionSpec as P

MESH = pl.DeviceIdType.MESH
HIST = 5
ITERS = 2
EPS = 0.1
LOG2E = math.log2(math.e)
INV = LOG2E / EPS
BACK = EPS * math.log(2.0)
LANES = 128
F32 = jnp.float32
BF16 = jnp.bfloat16


def rounded(value):
    return value.astype(BF16).astype(F32)


def split3(value):
    first = rounded(value)
    second = rounded(value - first)
    return first, second, rounded(value - first - second)


def select_rows(shape, rows):
    at = lax.broadcasted_iota(jnp.int32, shape, 0)
    out = jnp.zeros(shape, F32)
    for index, row in rows:
        out = jnp.where(at == index, row, out)
    return out


def solve_small(rows_list, values):
    extent = len(values)
    rows_list = [list(row) for row in rows_list]
    values = list(values)
    for pivot in range(extent):
        for lower in range(pivot + 1, extent):
            factor = rows_list[lower][pivot] / rows_list[pivot][pivot]
            for at in range(pivot, extent):
                rows_list[lower][at] = rows_list[lower][at] - factor * rows_list[pivot][at]
            values[lower] = values[lower] - factor * values[pivot]
    answer = [None] * extent
    for pivot in reversed(range(extent)):
        running = values[pivot]
        for upper in range(pivot + 1, extent):
            running = running - rows_list[pivot][upper] * answer[upper]
        answer[pivot] = running / rows_list[pivot][pivot]
    return answer


def inner_extent(R):
    best = 1
    while best * best * 4 <= R and R % (best * 2) == 0:
        best *= 2
    return best


def kernel(
    R, C,
    src_ref, tgt_ref, la_ref, lb_ref, g_ref, hg_ref, hm_ref,
    f_ref, gout_ref,
    src_all, tgt_all, g_all, hm_all, xt, xlow, y_all, ysq, mrow, srow,
    rp_send, rp_all, cp_send, cp_all, mp_send, mp_all, ga_send, ga_all,
    s_src, r_src, s_tgt, r_tgt, s_g, r_g, s_hm, r_hm,
    s_rp, r_rp, s_cp, r_cp, s_mp, r_mp, s_ga, r_ga,
):
    row = lax.axis_index("row")
    col = lax.axis_index("col")
    depth, nsrc = src_ref.shape
    ntgt = tgt_ref.shape[1]
    nrow = C * nsrc
    kdim = 4 * depth
    itile = min(256, nrow)
    pending = []

    def to_row(k):
        return lax.rem(row + k, R)

    def to_col(k):
        return lax.rem(col + k, C)

    X = inner_extent(R)
    Z = R // X
    outer, inner = row // X, lax.rem(row, X)

    def place(k, m):
        return lax.rem(outer + k, Z) * X + lax.rem(inner + m, X)

    def send(src, dst, ssem, rsem, device):
        copy = pltpu.make_async_remote_copy(
            src_ref=src, dst_ref=dst, send_sem=ssem, recv_sem=rsem,
            device_id=device, device_id_type=MESH,
        )
        copy.start()
        pending.append(copy)

    def arrived(dst, ssem, rsem):
        pltpu.make_async_remote_copy(
            src_ref=dst, dst_ref=dst, send_sem=ssem, recv_sem=rsem,
            device_id=(row, col), device_id_type=MESH,
        ).wait_recv()

    for k in range(1, C):
        p = to_col(k)
        send(src_ref, src_all.at[col], s_src.at[p], r_src.at[col], (row, p))
    for k in range(1, R):
        p = to_row(k)
        send(g_ref, g_all.at[row], s_g.at[p], r_g.at[row], (p, col))
    for k in range(1, Z):
        p = place(k, 0)
        send(tgt_ref, tgt_all.at[row], s_tgt.at[p], r_tgt.at[row], (p, col))
    for k in range(1, X):
        p = place(0, k)
        send(tgt_ref, tgt_all.at[row], s_tgt.at[p], r_tgt.at[row], (p, col))
    for k in range(1, R):
        p = to_row(k)
        send(hm_ref, hm_all.at[row], s_hm.at[p], r_hm.at[row], (p, col))

    src_all[col] = src_ref[...]
    tgt_all[row] = tgt_ref[...]
    g_all[row] = g_ref[...]
    hm_all[row] = hm_ref[...]

    def build_x(c):
        x = src_all[c]
        scaled = x * (2.0 * INV)
        high = rounded(scaled)
        low = rounded(scaled - high)
        ones = select_rows((depth, nsrc), [(k, 1.0) for k in range(3)])
        whole = jnp.concatenate([high, high, low, ones], axis=0).T.astype(BF16)
        at = pl.ds(pl.multiple_of(c * nsrc, nsrc), nsrc)
        xt[0, at, :] = whole
        xt[1, at, :] = whole
        xlow[c] = low
        return jnp.sum(x * x, axis=0, keepdims=True)

    def bias_y(p, g):
        bias = INV * g + LOG2E * lb_ref[pl.ds(p, 1), :] - INV * ysq[p]
        b1, b2, b3 = split3(bias)
        rows = [(0, b1), (1, b2), (2, b3)] + [(k, 1.0) for k in range(3, 6)]
        y_all[p, 3 * depth : 3 * depth + 16, :] = select_rows((16, ntgt), rows).astype(BF16)

    def build_y(p):
        y = tgt_all[p]
        high = y.astype(BF16)
        low = (y - high.astype(F32)).astype(BF16)
        y_all[p, 0:depth, :] = high
        y_all[p, depth : 2 * depth, :] = low
        y_all[p, 2 * depth : 3 * depth, :] = high
        y_all[p, 3 * depth + 16 :, :] = jnp.zeros((depth - 16, ntgt), BF16)
        ysq[p] = jnp.sum(y * y, axis=0, keepdims=True)
        bias_y(p, g_all[p])

    def row_chunk(p):
        for it in range(nrow // itile):
            at = slice(it * itile, (it + 1) * itile)
            s = jnp.dot(xt[0, at, :], y_all[p], preferred_element_type=F32)
            pieces = [s[:, k : k + LANES] for k in range(0, ntgt, LANES)]
            old = mrow[at, :]
            top = functools.reduce(jnp.maximum, pieces, old)
            total = srow[at, :] * jnp.exp2(old - top)
            for piece in pieces:
                total = total + jnp.exp2(piece - top)
            mrow[at, :] = top
            srow[at, :] = total

    def row_finish(turn):
        for at in range(0, nrow, LANES):
            mt = mrow[at : at + LANES, :].T
            st = srow[at : at + LANES, :].T
            top = jnp.max(mt, axis=0, keepdims=True)
            total = jnp.sum(st * jnp.exp2(mt - top), axis=0, keepdims=True)
            rp_send[turn, 0:1, at : at + LANES] = top
            rp_send[turn, 1:2, at : at + LANES] = total
        for k in range(1, C):
            p = to_col(k)
            send(rp_send.at[turn], rp_all.at[turn, col], s_rp.at[turn, p], r_rp.at[turn, col], (row, p))
        rp_all[turn, col] = rp_send[turn]
        for k in range(1, C):
            p = to_col(k)
            arrived(rp_all.at[turn, p], s_rp.at[turn, p], r_rp.at[turn, p])
        tops = [rp_all[turn, c, 0:1, :] for c in range(C)]
        top = functools.reduce(jnp.maximum, tops)
        total = jnp.zeros_like(top)
        for c in range(C):
            total = total + rp_all[turn, c, 1:2, :] * jnp.exp2(tops[c] - top)
        return top + jnp.log2(total)

    def set_row_term(lse):
        a1, a2, a3 = split3(LOG2E * la_ref[...] - lse)
        for c in range(C):
            at = slice(c * nsrc, (c + 1) * nsrc)
            rows = [(3, a1[:, at]), (4, a2[:, at]), (5, a3[:, at])]
            slab = jnp.concatenate([xlow[c], select_rows((depth, nsrc), rows)], axis=0)
            xt[1, at, 2 * depth :] = slab.T.astype(BF16)

    def col_chunk(turn, p):
        top = jnp.full((8, ntgt), -jnp.inf, F32)
        total = jnp.zeros((8, ntgt), F32)
        for it in range(nrow // itile):
            at = slice(it * itile, (it + 1) * itile)
            s = jnp.dot(xt[1, at, :], y_all[p], preferred_element_type=F32)
            s = s.reshape(itile // 8, 8, ntgt)
            new = jnp.maximum(top, jnp.max(s, axis=0))
            total = total * jnp.exp2(top - new) + jnp.sum(jnp.exp2(s - new[None]), axis=0)
            top = new
        best = jnp.max(top, axis=0, keepdims=True)
        cp_send[turn, p, 0:1, :] = best
        cp_send[turn, p, 1:2, :] = jnp.sum(total * jnp.exp2(top - best), axis=0, keepdims=True)

    def zero_bias(p, carry):
        at = lax.broadcasted_iota(jnp.int32, (16, ntgt), 0)
        one = jnp.where((at >= 3) & (at < 6), 1.0, 0.0)
        y_all[p, 3 * depth : 3 * depth + 16, :] = one.astype(BF16)
        return carry

    def reset_rows():
        mrow[...] = jnp.full(mrow.shape, -jnp.inf, F32)
        srow[...] = jnp.zeros(srow.shape, F32)

    reset_rows()
    for k in range(1, C):
        p = to_col(k)
        arrived(src_all.at[p], s_src.at[p], r_src.at[p])
    xsq = jnp.concatenate([build_x(c) for c in range(C)], axis=1)

    potentials = [hg_ref[k : k + 1, :] for k in range(hg_ref.shape[0])]
    images = [hm_ref[k : k + 1, :] for k in range(hm_ref.shape[0])]
    g_share = g_ref[...]
    own = tgt_ref[...]
    own_sq = jnp.sum(own * own, axis=0, keepdims=True)
    pairs = [(i, j) for i in range(HIST) for j in range(i, HIST)]
    grows = -(-len(pairs) // 8) * 8
    for turn in range(ITERS):
        if turn == 0:
            build_y(row)
            row_chunk(row)

            def take(p):
                arrived(g_all.at[p], s_g.at[p], r_g.at[p])
                build_y(p)
                row_chunk(p)

            def passed_on(p, q):
                return pltpu.make_async_remote_copy(
                    src_ref=tgt_all.at[p], dst_ref=tgt_all.at[p],
                    send_sem=s_tgt.at[q], recv_sem=r_tgt.at[p],
                    device_id=(row - inner + lax.rem(q, X), col),
                    device_id_type=MESH,
                )

            def first(k, carry):
                p = place(k, 0)
                arrived(tgt_all.at[p], s_tgt.at[p], r_tgt.at[p])
                for m in range(1, X):
                    passed_on(p, place(k, m)).start()
                take(p)
                return carry

            lax.fori_loop(1, Z, first, 0)

            def rest(n, carry):
                p = place(n // (X - 1), 1 + lax.rem(n, X - 1))
                arrived(tgt_all.at[p], s_tgt.at[p], r_tgt.at[p])
                take(p)
                return carry

            if X > 1:
                lax.fori_loop(0, Z * (X - 1), rest, 0)
            for k in range(1, Z):
                for m in range(1, X):
                    passed_on(place(k, 0), place(k, m)).wait_send()
        else:
            reset_rows()

            def again(p, carry):
                row_chunk(p)
                return carry

            lax.fori_loop(0, R, again, 0)
        lse = row_finish(turn)
        if turn == ITERS - 1:
            f_ref[...] = xsq - BACK * lse
        set_row_term(lse)
        lax.fori_loop(0, R, zero_bias, 0)

        def cols(k, carry):
            p = lax.rem(row + k, R)
            col_chunk(turn, p)
            pltpu.make_async_remote_copy(
                src_ref=cp_send.at[turn, p], dst_ref=cp_all.at[turn, row],
                send_sem=s_cp.at[turn, p], recv_sem=r_cp.at[turn, row],
                device_id=(p, col), device_id_type=MESH,
            ).start()
            return carry

        lax.fori_loop(1, R, cols, 0)
        col_chunk(turn, row)
        cp_all[turn, row] = cp_send[turn, row]
        for k in range(1, R):
            p = to_row(k)
            arrived(cp_all.at[turn, p], s_cp.at[turn, p], r_cp.at[turn, p])
        tops = [cp_all[turn, p, 0:1, :] for p in range(R)]
        best = functools.reduce(jnp.maximum, tops)
        total = jnp.zeros_like(best)
        for p in range(R):
            total = total + cp_all[turn, p, 1:2, :] * jnp.exp2(tops[p] - best)
        mapped = own_sq - BACK * (best + jnp.log2(total))
        potentials = (potentials + [g_share])[-HIST:]
        images = (images + [mapped])[-HIST:]
        resid = [a - b for a, b in zip(images, potentials)]
        lanes = lax.broadcasted_iota(jnp.int32, (1, LANES), 1)
        share = jnp.zeros((1, LANES), F32)
        for at, (i, j) in enumerate(pairs):
            share = jnp.where(lanes == at, jnp.sum(resid[i] * resid[j], axis=1, keepdims=True), share)
        ga_send[turn] = share
        me = row * C + col

        def gram_copy(n):
            d = lax.rem(me + n, R * C)
            return pltpu.make_async_remote_copy(
                src_ref=ga_send.at[turn], dst_ref=ga_all.at[turn, me],
                send_sem=s_ga.at[turn, d], recv_sem=r_ga.at[turn, me],
                device_id=(d // C, lax.rem(d, C)), device_id_type=MESH,
            )

        def gram_out(n, carry):
            gram_copy(n).start()
            return carry

        def gram_in(n, carry):
            d = lax.rem(me + n, R * C)
            arrived(ga_all.at[turn, d], s_ga.at[turn, d], r_ga.at[turn, d])
            return carry

        def gram_done(n, carry):
            gram_copy(n).wait_send()
            return carry

        lax.fori_loop(1, R * C, gram_out, 0)
        if turn < ITERS - 1:
            mp_send[turn] = mapped
            for k in range(1, R):
                p = to_row(k)
                send(mp_send.at[turn], mp_all.at[turn, row], s_mp.at[turn, p], r_mp.at[turn, row], (p, col))
            mp_all[turn, row] = mapped
        ga_all[turn, me] = share
        lax.fori_loop(1, R * C, gram_in, 0)
        gram = jnp.sum(ga_all[turn], axis=0)
        lax.fori_loop(1, R * C, gram_done, 0)
        wide = jnp.broadcast_to(gram, (grows, LANES))
        picked = lax.broadcasted_iota(jnp.int32, (grows, LANES), 0) == lax.broadcasted_iota(
            jnp.int32, (grows, LANES), 1
        )
        gram = jnp.sum(jnp.where(picked, wide, 0.0), axis=1, keepdims=True)
        gram = jnp.broadcast_to(gram, (grows, LANES))
        system = [[None] * HIST for _ in range(HIST)]
        for at, (i, j) in enumerate(pairs):
            system[i][j] = system[j][i] = gram[at : at + 1, :]
        trace = functools.reduce(jnp.add, [system[i][i] for i in range(HIST)])
        shift = 0.001 * trace / HIST + 1e-06
        for i in range(HIST):
            system[i][i] = system[i][i] + shift
        weights = solve_small(system, [jnp.ones((1, LANES), F32)] * HIST)
        norm = functools.reduce(jnp.add, weights)
        mix = [jnp.concatenate([w / norm] * (ntgt // LANES), axis=1) for w in weights]

        def mixed(parts):
            return functools.reduce(jnp.add, [w * part for w, part in zip(mix, parts)])

        g_share = mixed(images)
        if turn < ITERS - 1:
            if turn == 0:
                for k in range(1, R):
                    p = to_row(k)
                    arrived(hm_all.at[p], s_hm.at[p], r_hm.at[p])
            for k in range(1, R):
                p = to_row(k)
                arrived(mp_all.at[turn, p], s_mp.at[turn, p], r_mp.at[turn, p])
            for p in range(R):
                known = [hm_all[p, k : k + 1, :] for k in range(hm_ref.shape[0])]
                for past in range(turn + 1):
                    known.append(mp_all[past, p])
                bias_y(p, mixed(known[-HIST:]))
    gout_ref[...] = g_share
    for copy in pending:
        copy.wait_send()
    for turn in range(ITERS):
        for k in range(1, R):
            p = to_row(k)
            pltpu.make_async_remote_copy(
                src_ref=cp_send.at[turn, p], dst_ref=cp_all.at[turn, row],
                send_sem=s_cp.at[turn, p], recv_sem=r_cp.at[turn, row],
                device_id=(p, col), device_id_type=MESH,
            ).wait_send()


def shards(R, C, src, tgt, log_a, log_b, g_current, hist_g, hist_maps):
    depth, nsrc = src.shape
    ntgt = tgt.shape[1]
    nrow = C * nsrc
    nhist = hist_g.shape[0]
    dma = pltpu.SemaphoreType.DMA
    vmem = pl.BlockSpec(memory_space=pltpu.VMEM)
    f_out, g_out = pl.pallas_call(
        functools.partial(kernel, R, C),
        out_shape=(
            jax.ShapeDtypeStruct((1, nrow), F32),
            jax.ShapeDtypeStruct((1, ntgt), F32),
        ),
        in_specs=[vmem] * 7,
        out_specs=(vmem, vmem),
        scratch_shapes=[
            pltpu.VMEM((C, depth, nsrc), F32),
            pltpu.VMEM((R, depth, ntgt), F32),
            pltpu.VMEM((R, 1, ntgt), F32),
            pltpu.VMEM((R, nhist, ntgt), F32),
            pltpu.VMEM((2, nrow, 4 * depth), BF16),
            pltpu.VMEM((C, depth, nsrc), F32),
            pltpu.VMEM((R, 4 * depth, ntgt), BF16),
            pltpu.VMEM((R, 1, ntgt), F32),
            pltpu.VMEM((nrow, LANES), F32),
            pltpu.VMEM((nrow, LANES), F32),
            pltpu.VMEM((ITERS, 2, nrow), F32),
            pltpu.VMEM((ITERS, C, 2, nrow), F32),
            pltpu.VMEM((ITERS, R, 2, ntgt), F32),
            pltpu.VMEM((ITERS, R, 2, ntgt), F32),
            pltpu.VMEM((ITERS, 1, ntgt), F32),
            pltpu.VMEM((ITERS, R, 1, ntgt), F32),
            pltpu.VMEM((ITERS, 1, LANES), F32),
            pltpu.VMEM((ITERS, R * C, 1, LANES), F32),
            dma((C,)), dma((C,)), dma((R,)), dma((R,)),
            dma((R,)), dma((R,)), dma((R,)), dma((R,)),
            dma((ITERS, C)), dma((ITERS, C)), dma((ITERS, R)), dma((ITERS, R)),
            dma((ITERS, R)), dma((ITERS, R)), dma((ITERS, R * C)), dma((ITERS, R * C)),
        ],
        compiler_params=pltpu.CompilerParams(
            has_side_effects=True, vmem_limit_bytes=48 * 1024 * 1024
        ),
    )(
        src, tgt, log_a.reshape(1, nrow), log_b.reshape(R, ntgt),
        g_current.reshape(1, ntgt), hist_g, hist_maps,
    )
    return f_out.reshape(nrow), g_out.reshape(ntgt)


def solution(mesh):
    in_specs = (
        P(None, ("row", "col")),
        P(None, ("col", "row")),
        P("row"),
        P("col"),
        P(("col", "row")),
        P(None, ("col", "row")),
        P(None, ("col", "row")),
    )
    out_specs = (P("row"), P(("col", "row")))
    body = functools.partial(shards, mesh.shape["row"], mesh.shape["col"])
    return jax.shard_map(body, mesh=mesh, in_specs=in_specs, out_specs=out_specs, check_vma=False)
```

```python
import functools
import math

import jax
import jax.numpy as jnp
from jax import lax
from jax.experimental import pallas as pl
from jax.experimental.pallas import tpu as pltpu
from jax.sharding import PartitionSpec as P

MESH = pl.DeviceIdType.MESH
HIST = 5
ITERS = 2
EPS = 0.1
LOG2E = math.log2(math.e)
INV = LOG2E / EPS
BACK = EPS * math.log(2.0)
LANES = 128
F32 = jnp.float32
BF16 = jnp.bfloat16


def rounded(value):
    return value.astype(BF16).astype(F32)


def split3(value):
    first = rounded(value)
    second = rounded(value - first)
    return first, second, rounded(value - first - second)


def select_rows(shape, rows):
    at = lax.broadcasted_iota(jnp.int32, shape, 0)
    out = jnp.zeros(shape, F32)
    for index, row in rows:
        out = jnp.where(at == index, row, out)
    return out


def solve_small(rows_list, values):
    extent = len(values)
    rows_list = [list(row) for row in rows_list]
    values = list(values)
    for pivot in range(extent):
        for lower in range(pivot + 1, extent):
            factor = rows_list[lower][pivot] / rows_list[pivot][pivot]
            for at in range(pivot, extent):
                rows_list[lower][at] = rows_list[lower][at] - factor * rows_list[pivot][at]
            values[lower] = values[lower] - factor * values[pivot]
    answer = [None] * extent
    for pivot in reversed(range(extent)):
        running = values[pivot]
        for upper in range(pivot + 1, extent):
            running = running - rows_list[pivot][upper] * answer[upper]
        answer[pivot] = running / rows_list[pivot][pivot]
    return answer


def inner_extent(R):
    best = 1
    while best * best * 4 <= R and R % (best * 2) == 0:
        best *= 2
    return best


def kernel(
    R, C,
    src_ref, tgt_ref, la_ref, lb_ref, g_ref, hg_ref, hm_ref,
    f_ref, gout_ref,
    src_all, tgt_all, g_all, hm_all, xt, xlow, y_all, ysq, mrow, srow,
    rp_send, rp_all, cp_send, cp_all, mp_send, mp_all, ga_send, ga_all,
    s_src, r_src, s_tgt, r_tgt, s_g, r_g, s_hm, r_hm,
    s_rp, r_rp, s_cp, r_cp, s_mp, r_mp, s_ga, r_ga,
):
    row = lax.axis_index("row")
    col = lax.axis_index("col")
    depth, nsrc = src_ref.shape
    ntgt = tgt_ref.shape[1]
    nrow = C * nsrc
    kdim = 4 * depth
    itile = min(256, nrow)
    pending = []

    def to_row(k):
        return lax.rem(row + k, R)

    def to_col(k):
        return lax.rem(col + k, C)

    X = inner_extent(R)
    Z = R // X
    outer, inner = row // X, lax.rem(row, X)

    def partner(k):
        if Z & (Z - 1):
            return lax.rem(outer + k, Z)
        at = outer
        bit = 1
        while bit < Z:
            on = (k // bit) % 2 if isinstance(k, int) else lax.rem(k // bit, 2)
            at = at + on * bit * (1 - 2 * lax.rem(outer // bit, 2))
            bit *= 2
        return at

    def place(k, m):
        return partner(k) * X + lax.rem(inner + m, X)

    def send(src, dst, ssem, rsem, device):
        copy = pltpu.make_async_remote_copy(
            src_ref=src, dst_ref=dst, send_sem=ssem, recv_sem=rsem,
            device_id=device, device_id_type=MESH,
        )
        copy.start()
        pending.append(copy)

    def arrived(dst, ssem, rsem):
        pltpu.make_async_remote_copy(
            src_ref=dst, dst_ref=dst, send_sem=ssem, recv_sem=rsem,
            device_id=(row, col), device_id_type=MESH,
        ).wait_recv()

    for k in range(1, C):
        p = to_col(k)
        send(src_ref, src_all.at[col], s_src.at[p], r_src.at[col], (row, p))
    for k in range(1, R):
        p = to_row(k)
        send(g_ref, g_all.at[row], s_g.at[p], r_g.at[row], (p, col))
    for k in range(1, Z):
        p = place(k, 0)
        send(tgt_ref, tgt_all.at[row], s_tgt.at[p], r_tgt.at[row], (p, col))
    for k in range(1, X):
        p = place(0, k)
        send(tgt_ref, tgt_all.at[row], s_tgt.at[p], r_tgt.at[row], (p, col))
    for k in range(1, R):
        p = to_row(k)
        send(hm_ref, hm_all.at[row], s_hm.at[p], r_hm.at[row], (p, col))

    src_all[col] = src_ref[...]
    tgt_all[row] = tgt_ref[...]
    g_all[row] = g_ref[...]
    hm_all[row] = hm_ref[...]

    def build_x(c):
        x = src_all[c]
        scaled = x * (2.0 * INV)
        high = rounded(scaled)
        low = rounded(scaled - high)
        ones = select_rows((depth, nsrc), [(k, 1.0) for k in range(3)])
        whole = jnp.concatenate([high, high, low, ones], axis=0).T.astype(BF16)
        at = pl.ds(pl.multiple_of(c * nsrc, nsrc), nsrc)
        xt[0, at, :] = whole
        xt[1, at, :] = whole
        xlow[c] = low
        return jnp.sum(x * x, axis=0, keepdims=True)

    def bias_y(p, g):
        bias = INV * g + LOG2E * lb_ref[pl.ds(p, 1), :] - INV * ysq[p]
        b1, b2, b3 = split3(bias)
        rows = [(0, b1), (1, b2), (2, b3)] + [(k, 1.0) for k in range(3, 6)]
        y_all[p, 3 * depth : 3 * depth + 16, :] = select_rows((16, ntgt), rows).astype(BF16)

    def build_y(p):
        y = tgt_all[p]
        high = y.astype(BF16)
        low = (y - high.astype(F32)).astype(BF16)
        y_all[p, 0:depth, :] = high
        y_all[p, depth : 2 * depth, :] = low
        y_all[p, 2 * depth : 3 * depth, :] = high
        y_all[p, 3 * depth + 16 :, :] = jnp.zeros((depth - 16, ntgt), BF16)
        ysq[p] = jnp.sum(y * y, axis=0, keepdims=True)
        bias_y(p, g_all[p])

    def row_chunk(p):
        for it in range(nrow // itile):
            at = slice(it * itile, (it + 1) * itile)
            s = jnp.dot(xt[0, at, :], y_all[p], preferred_element_type=F32)
            pieces = [s[:, k : k + LANES] for k in range(0, ntgt, LANES)]
            old = mrow[at, :]
            top = functools.reduce(jnp.maximum, pieces, old)
            total = srow[at, :] * jnp.exp2(old - top)
            for piece in pieces:
                total = total + jnp.exp2(piece - top)
            mrow[at, :] = top
            srow[at, :] = total

    def row_finish(turn):
        for at in range(0, nrow, LANES):
            mt = mrow[at : at + LANES, :].T
            st = srow[at : at + LANES, :].T
            top = jnp.max(mt, axis=0, keepdims=True)
            total = jnp.sum(st * jnp.exp2(mt - top), axis=0, keepdims=True)
            rp_send[turn, 0:1, at : at + LANES] = top
            rp_send[turn, 1:2, at : at + LANES] = total
        for k in range(1, C):
            p = to_col(k)
            send(rp_send.at[turn], rp_all.at[turn, col], s_rp.at[turn, p], r_rp.at[turn, col], (row, p))
        rp_all[turn, col] = rp_send[turn]
        for k in range(1, C):
            p = to_col(k)
            arrived(rp_all.at[turn, p], s_rp.at[turn, p], r_rp.at[turn, p])
        tops = [rp_all[turn, c, 0:1, :] for c in range(C)]
        top = functools.reduce(jnp.maximum, tops)
        total = jnp.zeros_like(top)
        for c in range(C):
            total = total + rp_all[turn, c, 1:2, :] * jnp.exp2(tops[c] - top)
        return top + jnp.log2(total)

    def set_row_term(lse):
        a1, a2, a3 = split3(LOG2E * la_ref[...] - lse)
        for c in range(C):
            at = slice(c * nsrc, (c + 1) * nsrc)
            rows = [(3, a1[:, at]), (4, a2[:, at]), (5, a3[:, at])]
            slab = jnp.concatenate([xlow[c], select_rows((depth, nsrc), rows)], axis=0)
            xt[1, at, 2 * depth :] = slab.T.astype(BF16)

    def col_chunk(turn, p):
        top = jnp.full((8, ntgt), -jnp.inf, F32)
        total = jnp.zeros((8, ntgt), F32)
        for it in range(nrow // itile):
            at = slice(it * itile, (it + 1) * itile)
            s = jnp.dot(xt[1, at, :], y_all[p], preferred_element_type=F32)
            s = s.reshape(itile // 8, 8, ntgt)
            new = jnp.maximum(top, jnp.max(s, axis=0))
            total = total * jnp.exp2(top - new) + jnp.sum(jnp.exp2(s - new[None]), axis=0)
            top = new
        best = jnp.max(top, axis=0, keepdims=True)
        cp_send[turn, p, 0:1, :] = best
        cp_send[turn, p, 1:2, :] = jnp.sum(total * jnp.exp2(top - best), axis=0, keepdims=True)

    def zero_bias(p, carry):
        at = lax.broadcasted_iota(jnp.int32, (16, ntgt), 0)
        one = jnp.where((at >= 3) & (at < 6), 1.0, 0.0)
        y_all[p, 3 * depth : 3 * depth + 16, :] = one.astype(BF16)
        return carry

    def reset_rows():
        mrow[...] = jnp.full(mrow.shape, -jnp.inf, F32)
        srow[...] = jnp.zeros(srow.shape, F32)

    reset_rows()
    for k in range(1, C):
        p = to_col(k)
        arrived(src_all.at[p], s_src.at[p], r_src.at[p])
    xsq = jnp.concatenate([build_x(c) for c in range(C)], axis=1)

    potentials = [hg_ref[k : k + 1, :] for k in range(hg_ref.shape[0])]
    images = [hm_ref[k : k + 1, :] for k in range(hm_ref.shape[0])]
    g_share = g_ref[...]
    own = tgt_ref[...]
    own_sq = jnp.sum(own * own, axis=0, keepdims=True)
    pairs = [(i, j) for i in range(HIST) for j in range(i, HIST)]
    grows = -(-len(pairs) // 8) * 8
    for turn in range(ITERS):
        if turn == 0:
            build_y(row)
            row_chunk(row)

            def take(p):
                arrived(g_all.at[p], s_g.at[p], r_g.at[p])
                build_y(p)
                row_chunk(p)

            def passed_on(p, q):
                return pltpu.make_async_remote_copy(
                    src_ref=tgt_all.at[p], dst_ref=tgt_all.at[p],
                    send_sem=s_tgt.at[q], recv_sem=r_tgt.at[p],
                    device_id=(row - inner + lax.rem(q, X), col),
                    device_id_type=MESH,
                )

            def first(k, carry):
                p = place(k, 0)
                arrived(tgt_all.at[p], s_tgt.at[p], r_tgt.at[p])
                for m in range(1, X):
                    passed_on(p, place(k, m)).start()
                take(p)
                return carry

            lax.fori_loop(1, Z, first, 0)

            def rest(n, carry):
                p = place(n // (X - 1), 1 + lax.rem(n, X - 1))
                arrived(tgt_all.at[p], s_tgt.at[p], r_tgt.at[p])
                take(p)
                return carry

            if X > 1:
                lax.fori_loop(0, Z * (X - 1), rest, 0)
            for k in range(1, Z):
                for m in range(1, X):
                    passed_on(place(k, 0), place(k, m)).wait_send()
        else:
            reset_rows()

            def again(p, carry):
                row_chunk(p)
                return carry

            lax.fori_loop(0, R, again, 0)
        lse = row_finish(turn)
        if turn == ITERS - 1:
            f_ref[...] = xsq - BACK * lse
        set_row_term(lse)
        lax.fori_loop(0, R, zero_bias, 0)

        def cols(k, carry):
            p = lax.rem(row + k, R)
            col_chunk(turn, p)
            pltpu.make_async_remote_copy(
                src_ref=cp_send.at[turn, p], dst_ref=cp_all.at[turn, row],
                send_sem=s_cp.at[turn, p], recv_sem=r_cp.at[turn, row],
                device_id=(p, col), device_id_type=MESH,
            ).start()
            return carry

        lax.fori_loop(1, R, cols, 0)
        col_chunk(turn, row)
        cp_all[turn, row] = cp_send[turn, row]
        for k in range(1, R):
            p = to_row(k)
            arrived(cp_all.at[turn, p], s_cp.at[turn, p], r_cp.at[turn, p])
        tops = [cp_all[turn, p, 0:1, :] for p in range(R)]
        best = functools.reduce(jnp.maximum, tops)
        total = jnp.zeros_like(best)
        for p in range(R):
            total = total + cp_all[turn, p, 1:2, :] * jnp.exp2(tops[p] - best)
        mapped = own_sq - BACK * (best + jnp.log2(total))
        potentials = (potentials + [g_share])[-HIST:]
        images = (images + [mapped])[-HIST:]
        resid = [a - b for a, b in zip(images, potentials)]
        lanes = lax.broadcasted_iota(jnp.int32, (1, LANES), 1)
        share = jnp.zeros((1, LANES), F32)
        for at, (i, j) in enumerate(pairs):
            share = jnp.where(lanes == at, jnp.sum(resid[i] * resid[j], axis=1, keepdims=True), share)
        ga_send[turn] = share
        me = row * C + col

        def gram_copy(n):
            d = lax.rem(me + n, R * C)
            return pltpu.make_async_remote_copy(
                src_ref=ga_send.at[turn], dst_ref=ga_all.at[turn, me],
                send_sem=s_ga.at[turn, d], recv_sem=r_ga.at[turn, me],
                device_id=(d // C, lax.rem(d, C)), device_id_type=MESH,
            )

        def gram_out(n, carry):
            gram_copy(n).start()
            return carry

        def gram_in(n, carry):
            d = lax.rem(me + n, R * C)
            arrived(ga_all.at[turn, d], s_ga.at[turn, d], r_ga.at[turn, d])
            return carry

        def gram_done(n, carry):
            gram_copy(n).wait_send()
            return carry

        lax.fori_loop(1, R * C, gram_out, 0)
        if turn < ITERS - 1:
            mp_send[turn] = mapped
            for k in range(1, R):
                p = to_row(k)
                send(mp_send.at[turn], mp_all.at[turn, row], s_mp.at[turn, p], r_mp.at[turn, row], (p, col))
            mp_all[turn, row] = mapped
        ga_all[turn, me] = share
        lax.fori_loop(1, R * C, gram_in, 0)
        gram = jnp.sum(ga_all[turn], axis=0)
        lax.fori_loop(1, R * C, gram_done, 0)
        wide = jnp.broadcast_to(gram, (grows, LANES))
        picked = lax.broadcasted_iota(jnp.int32, (grows, LANES), 0) == lax.broadcasted_iota(
            jnp.int32, (grows, LANES), 1
        )
        gram = jnp.sum(jnp.where(picked, wide, 0.0), axis=1, keepdims=True)
        gram = jnp.broadcast_to(gram, (grows, LANES))
        system = [[None] * HIST for _ in range(HIST)]
        for at, (i, j) in enumerate(pairs):
            system[i][j] = system[j][i] = gram[at : at + 1, :]
        trace = functools.reduce(jnp.add, [system[i][i] for i in range(HIST)])
        shift = 0.001 * trace / HIST + 1e-06
        for i in range(HIST):
            system[i][i] = system[i][i] + shift
        weights = solve_small(system, [jnp.ones((1, LANES), F32)] * HIST)
        norm = functools.reduce(jnp.add, weights)
        mix = [jnp.concatenate([w / norm] * (ntgt // LANES), axis=1) for w in weights]

        def mixed(parts):
            return functools.reduce(jnp.add, [w * part for w, part in zip(mix, parts)])

        g_share = mixed(images)
        if turn < ITERS - 1:
            if turn == 0:
                for k in range(1, R):
                    p = to_row(k)
                    arrived(hm_all.at[p], s_hm.at[p], r_hm.at[p])
            for k in range(1, R):
                p = to_row(k)
                arrived(mp_all.at[turn, p], s_mp.at[turn, p], r_mp.at[turn, p])
            for p in range(R):
                known = [hm_all[p, k : k + 1, :] for k in range(hm_ref.shape[0])]
                for past in range(turn + 1):
                    known.append(mp_all[past, p])
                bias_y(p, mixed(known[-HIST:]))
    gout_ref[...] = g_share
    for copy in pending:
        copy.wait_send()
    for turn in range(ITERS):
        for k in range(1, R):
            p = to_row(k)
            pltpu.make_async_remote_copy(
                src_ref=cp_send.at[turn, p], dst_ref=cp_all.at[turn, row],
                send_sem=s_cp.at[turn, p], recv_sem=r_cp.at[turn, row],
                device_id=(p, col), device_id_type=MESH,
            ).wait_send()


def shards(R, C, src, tgt, log_a, log_b, g_current, hist_g, hist_maps):
    depth, nsrc = src.shape
    ntgt = tgt.shape[1]
    nrow = C * nsrc
    nhist = hist_g.shape[0]
    dma = pltpu.SemaphoreType.DMA
    vmem = pl.BlockSpec(memory_space=pltpu.VMEM)
    f_out, g_out = pl.pallas_call(
        functools.partial(kernel, R, C),
        out_shape=(
            jax.ShapeDtypeStruct((1, nrow), F32),
            jax.ShapeDtypeStruct((1, ntgt), F32),
        ),
        in_specs=[vmem] * 7,
        out_specs=(vmem, vmem),
        scratch_shapes=[
            pltpu.VMEM((C, depth, nsrc), F32),
            pltpu.VMEM((R, depth, ntgt), F32),
            pltpu.VMEM((R, 1, ntgt), F32),
            pltpu.VMEM((R, nhist, ntgt), F32),
            pltpu.VMEM((2, nrow, 4 * depth), BF16),
            pltpu.VMEM((C, depth, nsrc), F32),
            pltpu.VMEM((R, 4 * depth, ntgt), BF16),
            pltpu.VMEM((R, 1, ntgt), F32),
            pltpu.VMEM((nrow, LANES), F32),
            pltpu.VMEM((nrow, LANES), F32),
            pltpu.VMEM((ITERS, 2, nrow), F32),
            pltpu.VMEM((ITERS, C, 2, nrow), F32),
            pltpu.VMEM((ITERS, R, 2, ntgt), F32),
            pltpu.VMEM((ITERS, R, 2, ntgt), F32),
            pltpu.VMEM((ITERS, 1, ntgt), F32),
            pltpu.VMEM((ITERS, R, 1, ntgt), F32),
            pltpu.VMEM((ITERS, 1, LANES), F32),
            pltpu.VMEM((ITERS, R * C, 1, LANES), F32),
            dma((C,)), dma((C,)), dma((R,)), dma((R,)),
            dma((R,)), dma((R,)), dma((R,)), dma((R,)),
            dma((ITERS, C)), dma((ITERS, C)), dma((ITERS, R)), dma((ITERS, R)),
            dma((ITERS, R)), dma((ITERS, R)), dma((ITERS, R * C)), dma((ITERS, R * C)),
        ],
        compiler_params=pltpu.CompilerParams(
            has_side_effects=True, vmem_limit_bytes=48 * 1024 * 1024
        ),
    )(
        src, tgt, log_a.reshape(1, nrow), log_b.reshape(R, ntgt),
        g_current.reshape(1, ntgt), hist_g, hist_maps,
    )
    return f_out.reshape(nrow), g_out.reshape(ntgt)


def solution(mesh):
    in_specs = (
        P(None, ("row", "col")),
        P(None, ("col", "row")),
        P("row"),
        P("col"),
        P(("col", "row")),
        P(None, ("col", "row")),
        P(None, ("col", "row")),
    )
    out_specs = (P("row"), P(("col", "row")))
    body = functools.partial(shards, mesh.shape["row"], mesh.shape["col"])
    return jax.shard_map(body, mesh=mesh, in_specs=in_specs, out_specs=out_specs, check_vma=False)
```
